32 devices in a mesh: blk: 16 (over z, y, x), slab: 2 (over core).
Axes of the slice: x: 2, y: 2, z: 4, core: 2. Of those that a mesh axis runs over, the one named last changes fastest.
Arguments:
- sinogram: bfloat16 [32, 8, 2048], P('blk', 'slab'), parts along dimension 1, may hold values from -6 to 6
- jitter: bfloat16 [32], P('blk'), may hold values from -0.29882812 to 0.29882812
- shift: int32 [32], replicated, may hold values from -8 to 8
Outputs:
- image: float32 [32, 8, 2048], P('blk', 'slab'), parts along dimension 1
The draws below stay inside these ranges and needn't reach their ends.
There are 2 independent parts, one for each index of `slab`. The reference program is written for one: setup_inputs(seed, part) draws one part's arguments, and reference() takes and returns one part's arrays. A program takes and returns all parts, laid end to end along the dimension named above; an argument that names none is the same for every part. Nothing has to cross between parts.
All inputs are finite; a program needn't handle non-finite values.
Results may differ from the reference program's by a relative error of at most 0.0055.
Values may be sent and summed in bfloat16 or wider, within the bound.
No kernel may reach another device: no remote copies, remote signals or barrier semaphores. Data moves between devices by JAX's collectives and lax.ppermute only.
A program may use at most 64 MiB of HBM per device.

```python
import math
import jax
import jax.numpy as jnp
from jax import lax

BINS = 2048
SLICES = 4
ANGLES = 32
NROWS = 32


def place_ends(array, rng, smallest, top_value):
    index_at = [jax.random.randint(jax.random.fold_in(rng, axis), (), 0, length) for axis, length in enumerate(array.shape)]
    main_axis = array.shape.index(max(array.shape))
    beside = index_at[:main_axis] + [(index_at[main_axis] + 1) % array.shape[main_axis]] + index_at[main_axis + 1:]
    return array.at[tuple(index_at)].set(smallest).at[tuple(beside)].set(top_value)


def block_scale(rng, shape, split, smallest, high):
    def one(dim, shards_of):
        heights = jax.random.uniform(jax.random.fold_in(jax.random.fold_in(rng, 6), dim), (shards_of,), jnp.float32, smallest / len(split), high / len(split))
        return jnp.repeat(jnp.exp(heights), shape[dim] // shards_of).reshape((-1,) + (1,) * (len(shape) - dim - 1))

    level = one(*split[0])
    for cut in split[1:]:
        level = level * one(*cut)
    return level


def bell_draw(key, shape, deviation, most, pieces=(), held_as=jnp.bfloat16):
    entries = deviation * jax.random.normal(key, shape, jnp.float32)
    if pieces:
        entries = entries * block_scale(key, shape, pieces, -0.22, 0.18)
    return jnp.clip(entries, -most, most).astype(held_as)


def setup_inputs(seed: int = 0, part: int = 0) -> dict:
    splits = jax.random.split(jax.random.key(seed), 4)
    part_keys = jax.random.split(jax.random.fold_in(splits[3], part), 4)
    return {
        "sinogram": bell_draw(part_keys[0], (ANGLES, SLICES, BINS), 1.0, 6.0, ((0, 16),)),
        "jitter": jnp.clip(jax.random.uniform(splits[1], (ANGLES,), jnp.float32, -0.29882812, 0.29882812) * block_scale(splits[1], (ANGLES,), ((0, 16),), -0.4, 0.0), -0.29882812, 0.29882812).astype(jnp.bfloat16),
        "shift": place_ends(jax.random.randint(splits[2], (ANGLES,), -8, 9), jax.random.fold_in(splits[2], 1), -8, 8).astype(jnp.int32),
    }


def ramp_matrix(bins):
    offsets = jnp.arange(bins, dtype=jnp.int32)[None, :] - jnp.arange(bins, dtype=jnp.int32)[:, None]
    safe = jnp.where(offsets == 0, 1, offsets).astype(jnp.float32)
    odd_part = jnp.where(offsets % 2 != 0, -1.0 / (math.pi ** 2 * safe * safe), jnp.float32(0.0))
    kernel = jnp.where(offsets == 0, jnp.float32(0.25), odd_part)
    return kernel.astype(jnp.bfloat16)

def reference(sinogram, jitter, shift):
    ramp = ramp_matrix(BINS)
    jit_vals = jitter.astype(jnp.float32)
    weight = (1.0 + (jnp.roll(jit_vals, -1) - jnp.roll(jit_vals, 1)) * 1.5) * (4.0 / math.sqrt(ANGLES))
    flat = jnp.dot(sinogram.reshape(ANGLES * SLICES, BINS), ramp, preferred_element_type=jnp.float32)
    filtered = (flat.reshape(ANGLES, SLICES, BINS) * weight[:, None, None]).astype(jnp.bfloat16)
    padding = BINS // 4 + 192
    padded = jnp.pad(filtered, ((0, 0), (0, 0), (padding, padding))).astype(jnp.float32)
    theta = (jnp.arange(ANGLES, dtype=jnp.float32) + jit_vals) * math.pi / ANGLES
    cosine = jnp.cos(theta)
    sine_part = jnp.sin(theta)
    center_bin = (BINS - 1) / 2 + shift.astype(jnp.float32)
    coords_x = jnp.arange(BINS, dtype=jnp.float32) - (BINS - 1) / 2

    def one_row(row):
        row_pos = row.astype(jnp.float32) - (NROWS - 1) / 2
        coords = coords_x[None, :] * cosine[:, None] + row_pos * sine_part[:, None] + center_bin[:, None]
        lower = jnp.floor(coords)
        upper = lower + 1.0
        w_lower = jnp.maximum(0.0, 1.0 - jnp.abs(lower - coords)).astype(jnp.bfloat16).astype(jnp.float32)
        w_upper = jnp.maximum(0.0, 1.0 - jnp.abs(upper - coords)).astype(jnp.bfloat16).astype(jnp.float32)
        low_idx = lower.astype(jnp.int32) + padding
        idx_lo = jnp.broadcast_to(low_idx[:, None, :], (ANGLES, SLICES, BINS))
        f_lower = jnp.take_along_axis(padded, idx_lo, axis=2)
        f_upper = jnp.take_along_axis(padded, idx_lo + 1, axis=2)
        return lax.optimization_barrier(jnp.sum(f_lower * w_lower[:, None, :] + f_upper * w_upper[:, None, :], axis=0))
    return lax.map(one_row, jnp.arange(NROWS, dtype=jnp.int32))
```

```python
import functools
import math

import jax
import jax.numpy as jnp
from jax import lax
from jax.experimental import pallas as pl
from jax.experimental.pallas import tpu as pltpu
from jax.sharding import PartitionSpec as P

ROWS_DEV = 2
LANES = 128


def filter_kernel(sino_ref, jitter_ref, out_ref, ramp_ref):
    ang_dev, slices, bins = sino_ref.shape
    tiles = bins // LANES
    rows = ang_dev * slices
    lane = lax.broadcasted_iota(jnp.int32, (LANES, LANES), 1)
    row = lax.broadcasted_iota(jnp.int32, (LANES, LANES), 0)
    diff = lane - row
    odd = (diff & 1) == 1
    for d in range(2 * tiles - 1):
        n = diff + (d - tiles + 1) * LANES
        if d == tiles - 1:
            safe = jnp.where(n == 0, 1, n).astype(jnp.float32)
        else:
            safe = n.astype(jnp.float32)
        block = jnp.where(odd, -1.0 / (math.pi**2 * safe * safe), 0.0)
        if d == tiles - 1:
            block = jnp.where(n == 0, 0.25, block)
        ramp_ref[:, d * LANES : (d + 1) * LANES] = block.astype(jnp.bfloat16)
    sino = jnp.concatenate([sino_ref[a].astype(jnp.float32) for a in range(ang_dev)], axis=0)
    stacked = jnp.concatenate(
        [sino[:, i * LANES : (i + 1) * LANES] for i in range(tiles)], axis=0
    ).astype(jnp.bfloat16)
    parts = jnp.dot(stacked, ramp_ref[...], preferred_element_type=jnp.float32)
    for j in range(tiles):
        total = None
        for i in range(tiles):
            d = j - i + tiles - 1
            part = parts[i * rows : (i + 1) * rows, d * LANES : (d + 1) * LANES]
            total = part if total is None else total + part
        out_ref[:, j * LANES : (j + 1) * LANES] = total.astype(jnp.bfloat16)
    sub = lax.broadcasted_iota(jnp.int32, (rows, LANES), 0)
    spread = jnp.zeros((rows, LANES), jnp.float32)
    for a in range(ang_dev):
        value = jitter_ref[:, a : a + 1].astype(jnp.float32)
        spread = jnp.where(sub // slices == a, jnp.broadcast_to(value, (rows, LANES)), spread)
    out_ref[:, bins:] = spread.astype(jnp.bfloat16)


def project_kernel(
    here_ref, shift_ref, gath_ref, out_ref, val_ref, dif_ref, jit_ref, cos_ref, off_ref,
    tile_vmem, tile_smem, sem, *, nrows, bins, slices
):
    width = gath_ref.shape[0]
    angles = 2 * width
    tiles = bins // LANES
    padded = tiles + 2
    here = here_ref[0]
    lane = lax.broadcasted_iota(jnp.int32, (8, LANES), 1)
    sub = lax.broadcasted_iota(jnp.int32, (8, LANES), 0)
    first_half = sub < slices
    last_lane = lane == LANES - 1
    lane_f = lane.astype(jnp.float32)
    half = (bins - 1) / 2
    row_first = (here * ROWS_DEV).astype(jnp.float32) - (nrows - 1) / 2
    row_pos = row_first + jnp.where(first_half, 0.0, 1.0)

    def both(x):
        other = pltpu.roll(x, slices, axis=0)
        return jnp.where(first_half, x, other), jnp.where(first_half, other, x)

    def spread_jitter(d, carry):
        one, two = both(gath_ref[d, :, bins:].astype(jnp.float32))
        jit_ref[2 * d] = one
        jit_ref[2 * d + 1] = two
        return carry

    lax.fori_loop(0, width, spread_jitter, 0)

    def prepare(d, carry):
        raw = gath_ref[d, :, bins:].astype(jnp.float32)
        position = (2 * d).astype(jnp.float32) + jnp.where(first_half, 0.0, 1.0)
        theta = (position + raw) * math.pi / angles
        cosines = both(jnp.cos(theta))
        sines = both(jnp.sin(theta))
        scales = []
        for p in range(2):
            a = 2 * d + p
            after = jit_ref[lax.rem(a + 1, angles)]
            before = jit_ref[lax.rem(a + angles - 1, angles)]
            scales.append((1.0 + (after - before) * 1.5) * (4.0 / math.sqrt(angles)))
            c, s = cosines[p], sines[p]
            center = half + LANES + shift_ref[a].astype(jnp.float32)
            off = row_pos * s + center
            cos_ref[a] = c
            off_ref[a] = (lane_f - half) * c + off
            lowest = (lane_f * LANES - half + jnp.where(c < 0, LANES - 1.0, 0.0)) * c + off
            lowest = jnp.minimum(lowest, pltpu.roll(lowest, slices, axis=0)) - 0.25
            first_tile = jnp.clip(lowest.astype(jnp.int32) >> 7, 0, padded - 2)
            tile_vmem[pl.ds(a, 1), :] = first_tile[0:1, :]
        zero = jnp.zeros((8, LANES), jnp.float32)
        current, moved = zero, zero
        for t in range(padded):
            if t + 1 < padded - 1:
                following = gath_ref[d, :, t * LANES : (t + 1) * LANES].astype(jnp.float32)
                following_moved = pltpu.roll(following, LANES - 1, axis=1)
            else:
                following, following_moved = zero, zero
            step = jnp.where(last_lane, following_moved, moved) - current
            values = both(current) if 0 < t < padded - 1 else (zero, zero)
            steps = both(step)
            for p in range(2):
                val_ref[(2 * d + p) * padded + t] = values[p] * scales[p]
                dif_ref[(2 * d + p) * padded + t] = steps[p] * scales[p]
            current, moved = following, following_moved
        return carry

    lax.fori_loop(0, width, prepare, 0)
    copy = pltpu.make_async_copy(tile_vmem, tile_smem, sem)
    copy.start()
    copy.wait()

    def one_angle(a, accum):
        c = cos_ref[a]
        start = off_ref[a]
        result = []
        for j in range(tiles):
            t = tile_smem[a, j]
            at = a * padded + t
            coord = start + c * float(j * LANES)
            lower = coord.astype(jnp.int32)
            frac = coord - lower.astype(jnp.float32)
            local = lower - t * LANES
            inner = local & (LANES - 1)
            near = local < LANES
            take = functools.partial(jnp.take_along_axis, axis=1, mode="promise_in_bounds")
            value = jnp.where(near, take(val_ref[at], inner), take(val_ref[at + 1], inner))
            step = jnp.where(near, take(dif_ref[at], inner), take(dif_ref[at + 1], inner))
            result.append(accum[j] + (value + frac * step))
        return tuple(result)

    init = tuple(jnp.zeros((8, LANES), jnp.float32) for _ in range(tiles))
    accum = lax.fori_loop(0, angles, one_angle, init)
    for j in range(tiles):
        for r in range(ROWS_DEV):
            out_ref[r, :, j * LANES : (j + 1) * LANES] = accum[j][r * slices : (r + 1) * slices]


def body(sinogram, jitter, shift):
    ang_dev, slices, bins = sinogram.shape
    width = lax.axis_size("blk")
    angles = width * ang_dev
    nrows = ROWS_DEV * width
    padded = bins // LANES + 2
    here = lax.axis_index("blk").astype(jnp.int32).reshape(1)
    payload = pl.pallas_call(
        filter_kernel,
        out_shape=jax.ShapeDtypeStruct((ang_dev * slices, bins + LANES), jnp.bfloat16),
        scratch_shapes=[pltpu.VMEM((LANES, (2 * (bins // LANES) - 1) * LANES), jnp.bfloat16)],
        name="filter",
    )(sinogram, jitter.reshape(1, ang_dev))
    gathered = lax.all_gather(payload, "blk", axis=0, tiled=False)
    return pl.pallas_call(
        functools.partial(project_kernel, nrows=nrows, bins=bins, slices=slices),
        in_specs=[
            pl.BlockSpec(memory_space=pltpu.SMEM),
            pl.BlockSpec(memory_space=pltpu.SMEM),
            pl.BlockSpec(memory_space=pltpu.VMEM),
        ],
        out_shape=jax.ShapeDtypeStruct((ROWS_DEV, slices, bins), jnp.float32),
        scratch_shapes=[
            pltpu.VMEM((angles * padded, 8, LANES), jnp.float32),
            pltpu.VMEM((angles * padded, 8, LANES), jnp.float32),
            pltpu.VMEM((angles, 8, LANES), jnp.float32),
            pltpu.VMEM((angles, 8, LANES), jnp.float32),
            pltpu.VMEM((angles, 8, LANES), jnp.float32),
            pltpu.VMEM((angles, LANES), jnp.int32),
            pltpu.SMEM((angles, LANES), jnp.int32),
            pltpu.SemaphoreType.DMA(()),
        ],
        name="project",
    )(here, shift, gathered)


def solution(mesh):
    in_specs = (P("blk", "slab", None), P("blk"), P())
    out_specs = P("blk", "slab", None)
    return jax.shard_map(body, mesh=mesh, in_specs=in_specs, out_specs=out_specs, check_vma=False)
```

```python
import functools
import math

import jax
import jax.numpy as jnp
from jax import lax
from jax.experimental import pallas as pl
from jax.experimental.pallas import tpu as pltpu
from jax.sharding import PartitionSpec as P

ROWS_DEV = 2
LANES = 128


def filter_kernel(sino_ref, jitter_ref, out_ref, ramp_ref):
    ang_dev, slices, bins = sino_ref.shape
    tiles = bins // LANES
    rows = ang_dev * slices
    lane = lax.broadcasted_iota(jnp.int32, (LANES, LANES), 1)
    row = lax.broadcasted_iota(jnp.int32, (LANES, LANES), 0)
    diff = lane - row
    odd = (diff & 1) == 1
    for d in range(2 * tiles - 1):
        n = diff + (d - tiles + 1) * LANES
        if d == tiles - 1:
            safe = jnp.where(n == 0, 1, n).astype(jnp.float32)
        else:
            safe = n.astype(jnp.float32)
        block = jnp.where(odd, -1.0 / (math.pi**2 * safe * safe), 0.0)
        if d == tiles - 1:
            block = jnp.where(n == 0, 0.25, block)
        ramp_ref[:, d * LANES : (d + 1) * LANES] = block.astype(jnp.bfloat16)
    sino = jnp.concatenate([sino_ref[a].astype(jnp.float32) for a in range(ang_dev)], axis=0)
    stacked = jnp.concatenate(
        [sino[:, i * LANES : (i + 1) * LANES] for i in range(tiles)], axis=0
    ).astype(jnp.bfloat16)
    parts = jnp.dot(stacked, ramp_ref[...], preferred_element_type=jnp.float32)
    for j in range(tiles):
        total = None
        for i in range(tiles):
            d = j - i + tiles - 1
            part = parts[i * rows : (i + 1) * rows, d * LANES : (d + 1) * LANES]
            total = part if total is None else total + part
        out_ref[:, j * LANES : (j + 1) * LANES] = total.astype(jnp.bfloat16)
    sub = lax.broadcasted_iota(jnp.int32, (rows, LANES), 0)
    spread = jnp.zeros((rows, LANES), jnp.float32)
    for a in range(ang_dev):
        value = jitter_ref[:, a : a + 1].astype(jnp.float32)
        spread = jnp.where(sub // slices == a, jnp.broadcast_to(value, (rows, LANES)), spread)
    out_ref[:, bins:] = spread.astype(jnp.bfloat16)


def lane_take(x, index):
    numbers = lax.GatherDimensionNumbers(
        offset_dims=(),
        collapsed_slice_dims=(1,),
        start_index_map=(1,),
        operand_batching_dims=(0,),
        start_indices_batching_dims=(0,),
    )
    return lax.gather(
        x, index[:, :, None], numbers, (1, 1), mode=lax.GatherScatterMode.PROMISE_IN_BOUNDS
    )


def project_kernel(here_ref, order_ref, shift_ref, *refs, pieces, nrows, bins, slices):
    piece_refs, out_ref = refs[:pieces], refs[pieces]
    val_ref, dif_ref, jit_ref, cos_ref, off_ref, low_ref = refs[pieces + 1 : pieces + 7]
    tile_vmem, tile_smem, sem = refs[pieces + 7 :]
    width = sum(ref.shape[0] for ref in piece_refs)
    angles = 2 * width
    tiles = bins // LANES
    padded = tiles + 2
    here = here_ref[0]
    lane = lax.broadcasted_iota(jnp.int32, (8, LANES), 1)
    sub = lax.broadcasted_iota(jnp.int32, (8, LANES), 0)
    first_half = sub < slices
    last_lane = lane == LANES - 1
    lane_f = lane.astype(jnp.float32)
    half = (bins - 1) / 2
    row_first = (here * ROWS_DEV).astype(jnp.float32) - (nrows - 1) / 2
    row_pos = row_first + jnp.where(first_half, 0.0, 1.0)

    def both(x):
        other = pltpu.roll(x, slices, axis=0)
        return jnp.where(first_half, x, other), jnp.where(first_half, other, x)

    def spread_jitter(i, carry, piece, at):
        one, two = both(piece[i, :, bins:].astype(jnp.float32))
        d = here ^ order_ref[at + i]
        jit_ref[2 * d] = one
        jit_ref[2 * d + 1] = two
        return carry

    def each_device(function):
        at = 0
        for piece in piece_refs:
            count = piece.shape[0]
            lax.fori_loop(0, count, functools.partial(function, piece=piece, at=at), 0)
            at += count

    each_device(spread_jitter)

    def prepare(i, carry, piece, at):
        d = here ^ order_ref[at + i]
        raw = piece[i, :, bins:].astype(jnp.float32)
        position = (2 * d).astype(jnp.float32) + jnp.where(first_half, 0.0, 1.0)
        theta = (position + raw) * math.pi / angles
        cosines = both(jnp.cos(theta))
        sines = both(jnp.sin(theta))
        scales = []
        for p in range(2):
            a = 2 * d + p
            after = jit_ref[lax.rem(a + 1, angles)]
            before = jit_ref[lax.rem(a + angles - 1, angles)]
            scales.append((1.0 + (after - before) * 1.5) * (4.0 / math.sqrt(angles)))
            c, s = cosines[p], sines[p]
            center = half + LANES + shift_ref[a].astype(jnp.float32)
            off = row_pos * s + center
            low = (jnp.where(c < 0, LANES - 1.0, 0.0) - half) * c + off
            cos_ref[a] = c
            off_ref[a] = (lane_f - half) * c + off
            low_ref[a] = low
            lowest = low + c * (lane_f * LANES)
            lowest = jnp.minimum(lowest, pltpu.roll(lowest, slices, axis=0))
            first_tile = jnp.clip(lowest.astype(jnp.int32) >> 7, 0, padded - 2)
            tile_vmem[pl.ds(a, 1), :] = first_tile[0:1, :]
        zero = jnp.zeros((8, LANES), jnp.float32)
        current, moved = zero, zero
        for t in range(padded):
            if t + 1 < padded - 1:
                following = piece[i, :, t * LANES : (t + 1) * LANES].astype(jnp.float32)
                following_moved = pltpu.roll(following, LANES - 1, axis=1)
            else:
                following, following_moved = zero, zero
            step = jnp.where(last_lane, following_moved, moved) - current
            values = both(current) if 0 < t < padded - 1 else (zero, zero)
            steps = both(step)
            for p in range(2):
                val_ref[(2 * d + p) * padded + t] = values[p] * scales[p]
                dif_ref[(2 * d + p) * padded + t] = steps[p] * scales[p]
            current, moved = following, following_moved
        return carry

    each_device(prepare)
    copy = pltpu.make_async_copy(tile_vmem, tile_smem, sem)
    copy.start()
    copy.wait()

    def one_angle(a, accum):
        c = cos_ref[a]
        start = off_ref[a]
        low = low_ref[a]
        result = []
        for j in range(tiles):
            t = tile_smem[a, j]
            at = a * padded + t
            along = c * float(j * LANES)
            coord = start + along
            bottom = (low + along).astype(jnp.int32)
            lower = jnp.minimum(coord.astype(jnp.int32), bottom + (LANES - 1))
            frac = coord - lower.astype(jnp.float32)
            near = lane >= bottom - t * LANES
            inner = lower & (LANES - 1)
            value = lane_take(jnp.where(near, val_ref[at], val_ref[at + 1]), inner)
            step = lane_take(jnp.where(near, dif_ref[at], dif_ref[at + 1]), inner)
            result.append(accum[j] + (value + frac * step))
        return tuple(result)

    init = tuple(jnp.zeros((8, LANES), jnp.float32) for _ in range(tiles))
    accum = lax.fori_loop(0, angles, one_angle, init)
    for j in range(tiles):
        for r in range(ROWS_DEV):
            out_ref[r, :, j * LANES : (j + 1) * LANES] = accum[j][r * slices : (r + 1) * slices]


def exchange(pieces, width, stride, group):
    return [
        lax.ppermute(pieces, "blk", [(i, i ^ (k * stride)) for i in range(width)])
        for k in range(1, group)
    ]


def body(sinogram, jitter, shift):
    ang_dev, slices, bins = sinogram.shape
    width = lax.axis_size("blk")
    angles = width * ang_dev
    nrows = ROWS_DEV * width
    padded = bins // LANES + 2
    here = lax.axis_index("blk").astype(jnp.int32).reshape(1)
    payload = pl.pallas_call(
        filter_kernel,
        out_shape=jax.ShapeDtypeStruct((ang_dev * slices, bins + LANES), jnp.bfloat16),
        scratch_shapes=[pltpu.VMEM((LANES, (2 * (bins // LANES) - 1) * LANES), jnp.bfloat16)],
        name="filter",
    )(sinogram, jitter.reshape(1, ang_dev))
    assert width & (width - 1) == 0
    group_bits = width.bit_length() - 1
    pieces = [payload[None]]
    order = [0]
    while group_bits:
        group = 4 if group_bits >= 2 else 2
        group_bits -= group.bit_length() - 1
        stride = 1 << group_bits
        held = pieces[0] if len(pieces) == 1 else jnp.concatenate(pieces, axis=0)
        order = [o ^ (k * stride) for k in range(group) for o in order]
        pieces = [held] + exchange(held, width, stride, group)
    order = jnp.asarray(order, jnp.int32)
    return pl.pallas_call(
        functools.partial(project_kernel, pieces=len(pieces), nrows=nrows, bins=bins, slices=slices),
        in_specs=[
            pl.BlockSpec(memory_space=pltpu.SMEM),
            pl.BlockSpec(memory_space=pltpu.SMEM),
            pl.BlockSpec(memory_space=pltpu.SMEM),
        ]
        + [pl.BlockSpec(memory_space=pltpu.VMEM)] * len(pieces),
        out_shape=jax.ShapeDtypeStruct((ROWS_DEV, slices, bins), jnp.float32),
        scratch_shapes=[
            pltpu.VMEM((angles * padded, 8, LANES), jnp.float32),
            pltpu.VMEM((angles * padded, 8, LANES), jnp.float32),
            pltpu.VMEM((angles, 8, LANES), jnp.float32),
            pltpu.VMEM((angles, 8, LANES), jnp.float32),
            pltpu.VMEM((angles, 8, LANES), jnp.float32),
            pltpu.VMEM((angles, 8, LANES), jnp.float32),
            pltpu.VMEM((angles, LANES), jnp.int32),
            pltpu.SMEM((angles, LANES), jnp.int32),
            pltpu.SemaphoreType.DMA(()),
        ],
        name="project",
    )(here, order, shift, *pieces)


def solution(mesh):
    in_specs = (P("blk", "slab", None), P("blk"), P())
    out_specs = P("blk", "slab", None)
    return jax.shard_map(body, mesh=mesh, in_specs=in_specs, out_specs=out_specs, check_vma=False)
```

```python
import functools
import math

import jax
import jax.numpy as jnp
from jax import lax
from jax.experimental import pallas as pl
from jax.experimental.pallas import tpu as pltpu
from jax.sharding import PartitionSpec as P

ROWS_DEV = 2
LANES = 128


def filter_kernel(sino_ref, jitter_ref, out_ref, ramp_ref):
    ang_dev, slices, bins = sino_ref.shape
    tiles = bins // LANES
    rows = ang_dev * slices
    lane = lax.broadcasted_iota(jnp.int32, (LANES, LANES), 1)
    row = lax.broadcasted_iota(jnp.int32, (LANES, LANES), 0)
    diff = lane - row
    odd = (diff & 1) == 1
    for d in range(2 * tiles - 1):
        n = diff + (d - tiles + 1) * LANES
        if d == tiles - 1:
            safe = jnp.where(n == 0, 1, n).astype(jnp.float32)
        else:
            safe = n.astype(jnp.float32)
        block = jnp.where(odd, -1.0 / (math.pi**2 * safe * safe), 0.0)
        if d == tiles - 1:
            block = jnp.where(n == 0, 0.25, block)
        ramp_ref[:, d * LANES : (d + 1) * LANES] = block.astype(jnp.bfloat16)
    sino = jnp.concatenate([sino_ref[a].astype(jnp.float32) for a in range(ang_dev)], axis=0)
    stacked = jnp.concatenate(
        [sino[:, i * LANES : (i + 1) * LANES] for i in range(tiles)], axis=0
    ).astype(jnp.bfloat16)
    parts = jnp.dot(stacked, ramp_ref[...], preferred_element_type=jnp.float32)
    for j in range(tiles):
        total = None
        for i in range(tiles):
            d = j - i + tiles - 1
            part = parts[i * rows : (i + 1) * rows, d * LANES : (d + 1) * LANES]
            total = part if total is None else total + part
        out_ref[:, j * LANES : (j + 1) * LANES] = total.astype(jnp.bfloat16)
    sub = lax.broadcasted_iota(jnp.int32, (rows, LANES), 0)
    spread = jnp.zeros((rows, LANES), jnp.float32)
    for a in range(ang_dev):
        value = jitter_ref[:, a : a + 1].astype(jnp.float32)
        spread = jnp.where(sub // slices == a, jnp.broadcast_to(value, (rows, LANES)), spread)
    out_ref[:, bins:] = spread.astype(jnp.bfloat16)


def lane_take(x, index):
    numbers = lax.GatherDimensionNumbers(
        offset_dims=(),
        collapsed_slice_dims=(1,),
        start_index_map=(1,),
        operand_batching_dims=(0,),
        start_indices_batching_dims=(0,),
    )
    return lax.gather(
        x, index[:, :, None], numbers, (1, 1), mode=lax.GatherScatterMode.PROMISE_IN_BOUNDS
    )


def project(
    here, order_ref, shift_ref, pieces, at, scratch, spread, emit, *, width, bins, slices
):
    val_ref, dif_ref, cos_ref, off_ref, low_ref, tile_vmem, tile_smem, sem = scratch
    angles = 2 * width
    nrows = ROWS_DEV * width
    tiles = bins // LANES
    padded = tiles + 2
    lane = lax.broadcasted_iota(jnp.int32, (8, LANES), 1)
    sub = lax.broadcasted_iota(jnp.int32, (8, LANES), 0)
    first_half = sub < slices
    last_lane = lane == LANES - 1
    lane_f = lane.astype(jnp.float32)
    half = (bins - 1) / 2
    row_first = (here * ROWS_DEV).astype(jnp.float32) - (nrows - 1) / 2
    row_pos = row_first + jnp.where(first_half, 0.0, 1.0)

    def both(x):
        other = pltpu.roll(x, slices, axis=0)
        return jnp.where(first_half, x, other), jnp.where(first_half, other, x)

    def prepare(i, carry, piece, first):
        d = here ^ order_ref[at + first + i]
        raw = piece[i, :, bins:].astype(jnp.float32)
        for p, jitter in enumerate(both(raw)):
            spread(d, p, first + i, jitter)
        position = (2 * d).astype(jnp.float32) + jnp.where(first_half, 0.0, 1.0)
        theta = (position + raw) * math.pi / angles
        cosines = both(jnp.cos(theta))
        sines = both(jnp.sin(theta))
        local = 2 * (first + i)
        for p in range(2):
            c, s = cosines[p], sines[p]
            center = half + LANES + shift_ref[2 * d + p].astype(jnp.float32)
            off = row_pos * s + center
            low = (jnp.where(c < 0, LANES - 1.0, 0.0) - half) * c + off
            cos_ref[local + p] = c
            off_ref[local + p] = (lane_f - half) * c + off
            low_ref[local + p] = low
            lowest = low + c * (lane_f * LANES)
            lowest = jnp.minimum(lowest, pltpu.roll(lowest, slices, axis=0))
            first_tile = jnp.clip(lowest.astype(jnp.int32) >> 7, 0, padded - 2)
            tile_vmem[pl.ds(local + p, 1), :] = first_tile[0:1, :]
        zero = jnp.zeros((8, LANES), jnp.float32)
        current, moved = zero, zero
        for t in range(padded):
            if t + 1 < padded - 1:
                following = piece[i, :, t * LANES : (t + 1) * LANES].astype(jnp.float32)
                following_moved = pltpu.roll(following, LANES - 1, axis=1)
            else:
                following, following_moved = zero, zero
            step = jnp.where(last_lane, following_moved, moved) - current
            values = both(current) if 0 < t < padded - 1 else (zero, zero)
            steps = both(step)
            for p in range(2):
                val_ref[(local + p) * padded + t] = values[p]
                dif_ref[(local + p) * padded + t] = steps[p]
            current, moved = following, following_moved
        return carry

    first = 0
    for piece in pieces:
        count = piece.shape[0]
        lax.fori_loop(0, count, functools.partial(prepare, piece=piece, first=first), 0)
        first += count
    copy = pltpu.make_async_copy(tile_vmem, tile_smem, sem)
    copy.start()
    copy.wait()

    def one_angle(a, accum):
        c = cos_ref[a]
        start = off_ref[a]
        low = low_ref[a]
        blocks = []
        for j in range(tiles):
            t = tile_smem[a, j]
            base = a * padded + t
            along = c * float(j * LANES)
            coord = start + along
            bottom = (low + along).astype(jnp.int32)
            lower = jnp.minimum(coord.astype(jnp.int32), bottom + (LANES - 1))
            frac = coord - lower.astype(jnp.float32)
            near = lane >= bottom - t * LANES
            inner = lower & (LANES - 1)
            value = lane_take(jnp.where(near, val_ref[base], val_ref[base + 1]), inner)
            step = lane_take(jnp.where(near, dif_ref[base], dif_ref[base + 1]), inner)
            blocks.append(value + frac * step)
        return emit(a, blocks, accum)

    return one_angle, 2 * first


def early_kernel(here_ref, order_ref, shift_ref, held_ref, rows_ref, jit_ref, *scratch, width, bins, slices):
    tiles = bins // LANES

    def spread(d, p, local, jitter):
        jit_ref[2 * local + p] = jitter

    def emit(a, blocks, carry):
        for j in range(tiles):
            rows_ref[a * tiles + j] = blocks[j]
        return carry

    one_angle, count = project(
        here_ref[0], order_ref, shift_ref, [held_ref], 0, scratch, spread, emit,
        width=width, bins=bins, slices=slices,
    )
    lax.fori_loop(0, count, one_angle, 0)


def late_kernel(here_ref, order_ref, shift_ref, rows_ref, held_jit_ref, *refs, pieces, width, bins, slices):
    piece_refs, out_ref, jit_ref, scratch = (
        refs[:pieces], refs[pieces], refs[pieces + 1], refs[pieces + 2 :]
    )
    here = here_ref[0]
    angles = 2 * width
    tiles = bins // LANES
    held = held_jit_ref.shape[0] // 2

    def weight(position, p):
        a = 2 * (here ^ order_ref[position]) + p
        after = jit_ref[lax.rem(a + 1, angles)]
        before = jit_ref[lax.rem(a + angles - 1, angles)]
        return (1.0 + (after - before) * 1.5) * (4.0 / math.sqrt(angles))

    def spread(d, p, local, jitter):
        jit_ref[2 * d + p] = jitter

    def emit(a, blocks, accum):
        scale = weight(held + (a >> 1), a & 1)
        return tuple(accum[j] + scale * blocks[j] for j in range(tiles))

    for i in range(held):
        d = here ^ order_ref[i]
        for p in range(2):
            jit_ref[2 * d + p] = held_jit_ref[2 * i + p]
    one_angle, count = project(
        here, order_ref, shift_ref, piece_refs, held, scratch, spread, emit,
        width=width, bins=bins, slices=slices,
    )

    def add_early(a, accum):
        scale = weight(a >> 1, a & 1)
        return tuple(accum[j] + scale * rows_ref[a * tiles + j] for j in range(tiles))

    accum = tuple(jnp.zeros((8, LANES), jnp.float32) for _ in range(tiles))
    accum = lax.fori_loop(0, 2 * held, add_early, accum)
    accum = lax.fori_loop(0, count, one_angle, accum)
    for j in range(tiles):
        for r in range(ROWS_DEV):
            out_ref[r, :, j * LANES : (j + 1) * LANES] = accum[j][r * slices : (r + 1) * slices]


def working_set(count, bins):
    blocks = (bins // LANES + 2) * count
    return [
        pltpu.VMEM((blocks, 8, LANES), jnp.float32),
        pltpu.VMEM((blocks, 8, LANES), jnp.float32),
        pltpu.VMEM((count, 8, LANES), jnp.float32),
        pltpu.VMEM((count, 8, LANES), jnp.float32),
        pltpu.VMEM((count, 8, LANES), jnp.float32),
        pltpu.VMEM((count, LANES), jnp.int32),
        pltpu.SMEM((count, LANES), jnp.int32),
        pltpu.SemaphoreType.DMA(()),
    ]


def exchange(pieces, width, stride, group):
    return [
        lax.ppermute(pieces, "blk", [(i, i ^ (k * stride)) for i in range(width)])
        for k in range(1, group)
    ]


def body(sinogram, jitter, shift):
    ang_dev, slices, bins = sinogram.shape
    width = lax.axis_size("blk")
    angles = width * ang_dev
    here = lax.axis_index("blk").astype(jnp.int32).reshape(1)
    payload = pl.pallas_call(
        filter_kernel,
        out_shape=jax.ShapeDtypeStruct((ang_dev * slices, bins + LANES), jnp.bfloat16),
        scratch_shapes=[pltpu.VMEM((LANES, (2 * (bins // LANES) - 1) * LANES), jnp.bfloat16)],
        name="filter",
    )(sinogram, jitter.reshape(1, ang_dev))
    assert width & (width - 1) == 0
    group_bits = width.bit_length() - 1
    pieces = [payload[None]]
    order = [0]
    while group_bits:
        group = 4 if group_bits >= 2 else 2
        group_bits -= group.bit_length() - 1
        stride = 1 << group_bits
        held = pieces[0] if len(pieces) == 1 else jnp.concatenate(pieces, axis=0)
        order = [o ^ (k * stride) for k in range(group) for o in order]
        pieces = [held] + exchange(held, width, stride, group)
    order = jnp.asarray(order, jnp.int32)
    held, rest = pieces[0], pieces[1:]
    early = 2 * held.shape[0]
    late = angles - early
    scalars = [pl.BlockSpec(memory_space=pltpu.SMEM)] * 3
    whole = pl.BlockSpec(memory_space=pltpu.VMEM)
    rows, held_jitter = pl.pallas_call(
        functools.partial(early_kernel, width=width, bins=bins, slices=slices),
        in_specs=scalars + [whole],
        out_specs=[whole, whole],
        out_shape=[
            jax.ShapeDtypeStruct((early * (bins // LANES), 8, LANES), jnp.float32),
            jax.ShapeDtypeStruct((early, 8, LANES), jnp.float32),
        ],
        scratch_shapes=working_set(early, bins),
        name="early",
    )(here, order, shift, held)
    return pl.pallas_call(
        functools.partial(late_kernel, pieces=len(rest), width=width, bins=bins, slices=slices),
        in_specs=scalars + [whole] * (2 + len(rest)),
        out_shape=jax.ShapeDtypeStruct((ROWS_DEV, slices, bins), jnp.float32),
        scratch_shapes=[pltpu.VMEM((angles, 8, LANES), jnp.float32)] + working_set(late, bins),
        name="late",
    )(here, order, shift, rows, held_jitter, *rest)


def solution(mesh):
    in_specs = (P("blk", "slab", None), P("blk"), P())
    out_specs = P("blk", "slab", None)
    return jax.shard_map(body, mesh=mesh, in_specs=in_specs, out_specs=out_specs, check_vma=False)
```

```python
import functools
import math

import jax
import jax.numpy as jnp
from jax import lax
from jax.experimental import pallas as pl
from jax.experimental.pallas import tpu as pltpu
from jax.sharding import PartitionSpec as P

ROWS_DEV = 2
LANES = 128


def filter_kernel(sino_ref, jitter_ref, out_ref, ramp_ref):
    ang_dev, slices, bins = sino_ref.shape
    tiles = bins // LANES
    rows = ang_dev * slices
    lane = lax.broadcasted_iota(jnp.int32, (LANES, LANES), 1)
    row = lax.broadcasted_iota(jnp.int32, (LANES, LANES), 0)
    diff = lane - row
    odd = (diff & 1) == 1
    for d in range(2 * tiles - 1):
        n = diff + (d - tiles + 1) * LANES
        if d == tiles - 1:
            safe = jnp.where(n == 0, 1, n).astype(jnp.float32)
        else:
            safe = n.astype(jnp.float32)
        block = jnp.where(odd, -1.0 / (math.pi**2 * safe * safe), 0.0)
        if d == tiles - 1:
            block = jnp.where(n == 0, 0.25, block)
        ramp_ref[:, d * LANES : (d + 1) * LANES] = block.astype(jnp.bfloat16)
    sino = jnp.concatenate([sino_ref[a].astype(jnp.float32) for a in range(ang_dev)], axis=0)
    stacked = jnp.concatenate(
        [sino[:, i * LANES : (i + 1) * LANES] for i in range(tiles)], axis=0
    ).astype(jnp.bfloat16)
    parts = jnp.dot(stacked, ramp_ref[...], preferred_element_type=jnp.float32)
    for j in range(tiles):
        total = None
        for i in range(tiles):
            d = j - i + tiles - 1
            part = parts[i * rows : (i + 1) * rows, d * LANES : (d + 1) * LANES]
            total = part if total is None else total + part
        out_ref[:, j * LANES : (j + 1) * LANES] = total.astype(jnp.bfloat16)
    sub = lax.broadcasted_iota(jnp.int32, (rows, LANES), 0)
    spread = jnp.zeros((rows, LANES), jnp.float32)
    for a in range(ang_dev):
        value = jitter_ref[:, a : a + 1].astype(jnp.float32)
        spread = jnp.where(sub // slices == a, jnp.broadcast_to(value, (rows, LANES)), spread)
    out_ref[:, bins:] = spread.astype(jnp.bfloat16)


def lane_take(x, index):
    numbers = lax.GatherDimensionNumbers(
        offset_dims=(),
        collapsed_slice_dims=(1,),
        start_index_map=(1,),
        operand_batching_dims=(0,),
        start_indices_batching_dims=(0,),
    )
    return lax.gather(
        x, index[:, :, None], numbers, (1, 1), mode=lax.GatherScatterMode.PROMISE_IN_BOUNDS
    )


def project(
    here, order_ref, shift_ref, pieces, at, scratch, spread, emit, *, width, bins, slices
):
    val_ref, dif_ref, cos_ref, off_ref, low_ref, tile_vmem, tile_smem, sem = scratch
    angles = 2 * width
    nrows = ROWS_DEV * width
    tiles = bins // LANES
    padded = tiles + 2
    lane = lax.broadcasted_iota(jnp.int32, (8, LANES), 1)
    sub = lax.broadcasted_iota(jnp.int32, (8, LANES), 0)
    first_half = sub < slices
    last_lane = lane == LANES - 1
    lane_f = lane.astype(jnp.float32)
    half = (bins - 1) / 2
    row_first = (here * ROWS_DEV).astype(jnp.float32) - (nrows - 1) / 2
    row_pos = row_first + jnp.where(first_half, 0.0, 1.0)

    def both(x):
        other = pltpu.roll(x, slices, axis=0)
        return jnp.where(first_half, x, other), jnp.where(first_half, other, x)

    def prepare(i, carry, piece, first):
        d = here ^ order_ref[at + first + i]
        raw = piece[i, :, bins:].astype(jnp.float32)
        for p, jitter in enumerate(both(raw)):
            spread(d, p, first + i, jitter)
        position = (2 * d).astype(jnp.float32) + jnp.where(first_half, 0.0, 1.0)
        theta = (position + raw) * math.pi / angles
        cosines = both(jnp.cos(theta))
        sines = both(jnp.sin(theta))
        local = 2 * (first + i)
        for p in range(2):
            c, s = cosines[p], sines[p]
            center = half + LANES + shift_ref[2 * d + p].astype(jnp.float32)
            off = row_pos * s + center
            low = (jnp.where(c < 0, LANES - 1.0, 0.0) - half) * c + off
            cos_ref[local + p] = c
            off_ref[local + p] = (lane_f - half) * c + off
            low_ref[local + p] = low
            lowest = low + c * (lane_f * LANES)
            lowest = jnp.minimum(lowest, pltpu.roll(lowest, slices, axis=0))
            first_tile = jnp.clip(lowest.astype(jnp.int32) >> 7, 0, padded - 2)
            tile_vmem[pl.ds(local + p, 1), :] = first_tile[0:1, :]
        zero = jnp.zeros((8, LANES), jnp.float32)
        current, moved = zero, zero
        for t in range(padded):
            if t + 1 < padded - 1:
                following = piece[i, :, t * LANES : (t + 1) * LANES].astype(jnp.float32)
                following_moved = pltpu.roll(following, LANES - 1, axis=1)
            else:
                following, following_moved = zero, zero
            step = jnp.where(last_lane, following_moved, moved) - current
            values = both(current) if 0 < t < padded - 1 else (zero, zero)
            steps = both(step)
            for p in range(2):
                val_ref[(local + p) * padded + t] = values[p]
                dif_ref[(local + p) * padded + t] = steps[p]
            current, moved = following, following_moved
        return carry

    first = 0
    for piece in pieces:
        count = piece.shape[0]
        lax.fori_loop(0, count, functools.partial(prepare, piece=piece, first=first), 0, unroll=2)
        first += count
    copy = pltpu.make_async_copy(tile_vmem, tile_smem, sem)
    copy.start()
    copy.wait()

    def one_angle(a, accum):
        c = cos_ref[a]
        start = off_ref[a]
        low = low_ref[a]
        blocks = []
        for j in range(tiles):
            t = tile_smem[a, j]
            base = a * padded + t
            along = c * float(j * LANES)
            coord = start + along
            bottom = (low + along).astype(jnp.int32)
            lower = jnp.minimum(coord.astype(jnp.int32), bottom + (LANES - 1))
            frac = coord - lower.astype(jnp.float32)
            near = lane >= bottom - t * LANES
            inner = lower & (LANES - 1)
            value = lane_take(jnp.where(near, val_ref[base], val_ref[base + 1]), inner)
            step = lane_take(jnp.where(near, dif_ref[base], dif_ref[base + 1]), inner)
            blocks.append(value + frac * step)
        return emit(a, blocks, accum)

    return one_angle, 2 * first


def early_kernel(here_ref, order_ref, shift_ref, held_ref, rows_ref, jit_ref, *scratch, width, bins, slices):
    tiles = bins // LANES

    def spread(d, p, local, jitter):
        jit_ref[2 * local + p] = jitter

    def emit(a, blocks, carry):
        for j in range(tiles):
            rows_ref[a * tiles + j] = blocks[j]
        return carry

    one_angle, count = project(
        here_ref[0], order_ref, shift_ref, [held_ref], 0, scratch, spread, emit,
        width=width, bins=bins, slices=slices,
    )
    lax.fori_loop(0, count, one_angle, 0, unroll=4)


def late_kernel(here_ref, order_ref, shift_ref, rows_ref, held_jit_ref, *refs, pieces, width, bins, slices):
    piece_refs, out_ref, jit_ref, scratch = (
        refs[:pieces], refs[pieces], refs[pieces + 1], refs[pieces + 2 :]
    )
    here = here_ref[0]
    angles = 2 * width
    tiles = bins // LANES
    held = held_jit_ref.shape[0] // 2

    def weight(position, p):
        a = 2 * (here ^ order_ref[position]) + p
        after = jit_ref[lax.rem(a + 1, angles)]
        before = jit_ref[lax.rem(a + angles - 1, angles)]
        return (1.0 + (after - before) * 1.5) * (4.0 / math.sqrt(angles))

    def spread(d, p, local, jitter):
        jit_ref[2 * d + p] = jitter

    def emit(a, blocks, accum):
        scale = weight(held + (a >> 1), a & 1)
        return tuple(accum[j] + scale * blocks[j] for j in range(tiles))

    for i in range(held):
        d = here ^ order_ref[i]
        for p in range(2):
            jit_ref[2 * d + p] = held_jit_ref[2 * i + p]
    one_angle, count = project(
        here, order_ref, shift_ref, piece_refs, held, scratch, spread, emit,
        width=width, bins=bins, slices=slices,
    )

    def add_early(a, accum):
        scale = weight(a >> 1, a & 1)
        return tuple(accum[j] + scale * rows_ref[a * tiles + j] for j in range(tiles))

    accum = tuple(jnp.zeros((8, LANES), jnp.float32) for _ in range(tiles))
    accum = lax.fori_loop(0, 2 * held, add_early, accum)
    accum = lax.fori_loop(0, count, one_angle, accum, unroll=4)
    for j in range(tiles):
        for r in range(ROWS_DEV):
            out_ref[r, :, j * LANES : (j + 1) * LANES] = accum[j][r * slices : (r + 1) * slices]


def working_set(count, bins):
    blocks = (bins // LANES + 2) * count
    return [
        pltpu.VMEM((blocks, 8, LANES), jnp.float32),
        pltpu.VMEM((blocks, 8, LANES), jnp.float32),
        pltpu.VMEM((count, 8, LANES), jnp.float32),
        pltpu.VMEM((count, 8, LANES), jnp.float32),
        pltpu.VMEM((count, 8, LANES), jnp.float32),
        pltpu.VMEM((count, LANES), jnp.int32),
        pltpu.SMEM((count, LANES), jnp.int32),
        pltpu.SemaphoreType.DMA(()),
    ]


def exchange(pieces, width, stride, group):
    return [
        lax.ppermute(pieces, "blk", [(i, i ^ (k * stride)) for i in range(width)])
        for k in range(1, group)
    ]


def body(sinogram, jitter, shift):
    ang_dev, slices, bins = sinogram.shape
    width = lax.axis_size("blk")
    angles = width * ang_dev
    here = lax.axis_index("blk").astype(jnp.int32).reshape(1)
    payload = pl.pallas_call(
        filter_kernel,
        out_shape=jax.ShapeDtypeStruct((ang_dev * slices, bins + LANES), jnp.bfloat16),
        scratch_shapes=[pltpu.VMEM((LANES, (2 * (bins // LANES) - 1) * LANES), jnp.bfloat16)],
        name="filter",
    )(sinogram, jitter.reshape(1, ang_dev))
    assert width & (width - 1) == 0
    group_bits = width.bit_length() - 1
    pieces = [payload[None]]
    order = [0]
    while group_bits:
        group = 4 if group_bits >= 2 else 2
        group_bits -= group.bit_length() - 1
        stride = 1 << group_bits
        held = pieces[0] if len(pieces) == 1 else jnp.concatenate(pieces, axis=0)
        order = [o ^ (k * stride) for k in range(group) for o in order]
        pieces = [held] + exchange(held, width, stride, group)
    order = jnp.asarray(order, jnp.int32)
    held, rest = pieces[0], pieces[1:]
    early = 2 * held.shape[0]
    late = angles - early
    scalars = [pl.BlockSpec(memory_space=pltpu.SMEM)] * 3
    whole = pl.BlockSpec(memory_space=pltpu.VMEM)
    rows, held_jitter = pl.pallas_call(
        functools.partial(early_kernel, width=width, bins=bins, slices=slices),
        in_specs=scalars + [whole],
        out_specs=[whole, whole],
        out_shape=[
            jax.ShapeDtypeStruct((early * (bins // LANES), 8, LANES), jnp.float32),
            jax.ShapeDtypeStruct((early, 8, LANES), jnp.float32),
        ],
        scratch_shapes=working_set(early, bins),
        name="early",
    )(here, order, shift, held)
    return pl.pallas_call(
        functools.partial(late_kernel, pieces=len(rest), width=width, bins=bins, slices=slices),
        in_specs=scalars + [whole] * (2 + len(rest)),
        out_shape=jax.ShapeDtypeStruct((ROWS_DEV, slices, bins), jnp.float32),
        scratch_shapes=[pltpu.VMEM((angles, 8, LANES), jnp.float32)] + working_set(late, bins),
        name="late",
    )(here, order, shift, rows, held_jitter, *rest)


def solution(mesh):
    in_specs = (P("blk", "slab", None), P("blk"), P())
    out_specs = P("blk", "slab", None)
    return jax.shard_map(body, mesh=mesh, in_specs=in_specs, out_specs=out_specs, check_vma=False)
```
